32 devices in a mesh: tm: 4 (over x, core), space: 8 (over z, y).
Axes of the slice: x: 2, y: 2, z: 4, core: 2. Of those that a mesh axis runs over, the one named last changes fastest.
Arguments:
- obs_perturb: bfloat16 [4, 32, 1024, 256], P('tm', 'space'), may hold values from -1.796875 to 1.796875
- innovation: float32 [4, 32, 1024], P('tm', 'space'), may hold values from -12 to 12
- error_weight: float32 [4, 32, 1024], P('tm', 'space'), may hold values from 0.5 to 2
- obs_column: int32 [4, 32, 1024], P('tm', 'space'), may hold values from 0 to 31
- obs_count: int32 [4, 32], P('tm', 'space'), may hold values from 64 to 1024, as said below
- radius: int32 [32], P('space'), may hold values from 56 to 80
- states: bfloat16 [8, 1024, 16, 256], P('tm', 'space'), may hold values from -6 to 6
Outputs:
- analysis: bfloat16 [8, 1024, 16, 256], P('tm', 'space')
The draws below stay inside these ranges and needn't reach their ends.
Inputs may be any that keep to these rules, and one draw needn't show every extreme that they name: `obs_count`: at most 1024; some slot and region holds exactly 1024 in every draw.
All inputs are finite; a program needn't handle non-finite values.
Results may differ from the reference program's by a relative error of at most 0.0065.
Values may be sent and summed in bfloat16 or wider, within the bound.
A program may use at most 64 MiB of HBM per device.

```python
import math
import jax
import jax.numpy as jnp
from jax import lax

K = 256
HC = 32
LEV = 16
OBS_CAP = 1024
NS_ITERS = 5
SLOTS = 4
LAGS = 8
REGIONS = 32
COLUMNS = 1024


def draw_obs_count(key, part):
    heavy_key, high_key, low_key, pick_key = jax.random.split(key, 4)
    grid_shape = (SLOTS, REGIONS)
    heavy_mask = jax.random.randint(heavy_key, grid_shape, 0, 4) == 0
    high_count = jax.random.randint(high_key, grid_shape, OBS_CAP // 2, OBS_CAP + 1)
    low_count = jax.random.randint(low_key, grid_shape, OBS_CAP // 16, OBS_CAP // 4 + 1)
    counts = jnp.where(heavy_mask, high_count, low_count).reshape(-1)
    chosen = jax.random.randint(pick_key, (), 0, SLOTS * REGIONS)
    counts = counts.at[chosen].set(OBS_CAP)
    return counts.reshape(grid_shape).astype(jnp.int32)


def place_ends(drawn, own_key, smallest, top_value):
    dims = drawn.shape
    place = [jax.random.randint(jax.random.fold_in(own_key, axis), (), 0, dims[axis]) for axis in range(len(dims))]
    drawn = drawn.at[tuple(place)].set(smallest)
    longest = dims.index(max(dims))
    place[longest] = (place[longest] + 1) % dims[longest]
    return drawn.at[tuple(place)].set(top_value)


def shard_levels(rng, dims, pieces, low, largest):
    level = 1.0
    for dim, blocks in pieces:
        draws = jax.random.uniform(jax.random.fold_in(jax.random.fold_in(rng, 6), dim), (blocks,), jnp.float32, low / len(pieces), largest / len(pieces))
        level = level * jnp.repeat(jnp.exp(draws), dims[dim] // blocks).reshape((-1,) + (1,) * (len(dims) - 1 - dim))
    return level


def centred(stream_key, extent, deviation, reach, pieces=(), held_as=jnp.bfloat16):
    gain = shard_levels(stream_key, extent, pieces, -0.22, 0.18) if pieces else 1.0
    entries = jax.random.normal(stream_key, extent, jnp.float32) * deviation * gain
    return jnp.minimum(jnp.maximum(entries, -reach), reach).astype(held_as)


def setup_inputs(seed: int = 0) -> dict:
    keys = jax.random.split(jax.random.key(seed), 8)
    return {
        "obs_perturb": centred(keys[0], (SLOTS, REGIONS, OBS_CAP, K), 0.3, 1.796875, ((0, 4), (1, 8))),
        "innovation": centred(keys[1], (SLOTS, REGIONS, OBS_CAP), 2.0, 12.0, ((0, 4), (1, 8)), jnp.float32),
        "error_weight": jnp.clip(jnp.exp(math.log(2.0) - 1.3862944 * jax.random.uniform(keys[2], (SLOTS, REGIONS, OBS_CAP), jnp.float32) ** shard_levels(keys[2], (SLOTS, REGIONS, OBS_CAP), ((0, 4), (1, 8)), -0.2, 0.2)), 0.5, 2.0),
        "obs_column": place_ends(jax.random.randint(keys[3], (SLOTS, REGIONS, OBS_CAP), 0, HC), jax.random.fold_in(keys[3], 1), 0, HC - 1).astype(jnp.int32),
        "obs_count": draw_obs_count(jax.random.fold_in(keys[7], 71), 0),
        "radius": place_ends(jax.random.randint(keys[5], (REGIONS,), 7 * HC // 4, 5 * HC // 2 + 1), jax.random.fold_in(keys[5], 1), 7 * HC // 4, (5 * HC // 2 + 1) - 1).astype(jnp.int32),
        "states": centred(keys[6], (LAGS, COLUMNS, LEV, K), 1.0, 6.0, ((0, 4), (1, 8))),
    }


INFLATION = 1.1
HIGHEST = lax.Precision.HIGHEST

def taper(column, radius, offset, width):
    distance = jnp.abs(column.astype(jnp.float32) + 0.5 - 0.5 * width - offset * width)
    ratio = jnp.minimum(distance / radius.astype(jnp.float32), 1.0)
    return jnp.square(1.0 - ratio * ratio)

def ensemble_transform(gram_sum, innov_sum):
    members = gram_sum.shape[-1]
    identity = jnp.eye(members, dtype=jnp.float32)
    system = gram_sum + (members - 1) / INFLATION * identity
    frobenius = jnp.sqrt(lax.optimization_barrier(jnp.sum(system * system, axis=(1, 2))))
    root_now = system / frobenius[:, None, None]
    inverse = jnp.broadcast_to(identity, system.shape)
    for iteration in range(NS_ITERS):
        middle = 1.5 * identity - 0.5 * jnp.einsum('nij,njk->nik', inverse, root_now, precision=HIGHEST)
        root_now = jnp.einsum('nij,njk->nik', root_now, middle, precision=HIGHEST)
        inverse = jnp.einsum('nij,njk->nik', middle, inverse, precision=HIGHEST)
    spread_part = jnp.sqrt(members - 1.0) * inverse / jnp.sqrt(frobenius)[:, None, None]
    half_step = jnp.einsum('nij,nj->ni', inverse, innov_sum, precision=HIGHEST)
    mean_part = jnp.einsum('nij,nj->ni', inverse, half_step, precision=HIGHEST) / frobenius[:, None]
    return spread_part + mean_part[:, :, None]

def reference(obs_perturb, innovation, error_weight, obs_column, obs_count, radius, states):
    slot_count, region_count, capacity, members = obs_perturb.shape
    position = lax.broadcasted_iota(jnp.int32, (slot_count, region_count, capacity), 2)
    present = (position < obs_count[:, :, None]).astype(jnp.float32)
    base_weight = error_weight * present
    weights = jnp.stack([base_weight * taper(obs_column, radius[None, :, None], offset, HC) for offset in range(-2, 3)])

    def region_gram(target):
        gram_sum = jnp.zeros((members, members), jnp.float32)
        vec_sum = jnp.zeros((members,), jnp.float32)
        for term_index, offset in enumerate(range(-2, 3)):
            source = (target - offset) % region_count
            source_rows = obs_perturb[:, source].reshape(-1, members)
            weight = weights[term_index][:, source].reshape(-1)
            weighted = (source_rows * weight[:, None]).astype(jnp.bfloat16)
            gram_sum = gram_sum + jnp.dot(weighted.T, source_rows, preferred_element_type=jnp.float32)
            vec_sum = vec_sum + jnp.dot(weighted.astype(jnp.float32).T, innovation[:, source].reshape(-1), precision=HIGHEST)
        return (gram_sum, vec_sum)
    gram_all, vec_all = lax.map(region_gram, jnp.arange(region_count, dtype=jnp.int32))
    transform = ensemble_transform(gram_all, vec_all).astype(jnp.bfloat16)
    preceding = jnp.roll(transform, 1, axis=0)
    following = jnp.roll(transform, -1, axis=0)
    lag_count = states.shape[0]
    levels = states.shape[2]
    shaped = states.reshape(lag_count, region_count, HC, levels, members)
    half_width = HC // 2
    blend_weight = jnp.abs((jnp.arange(HC, dtype=jnp.float32) + 0.5) / HC - 0.5).reshape(1, HC, 1, 1)

    def region_update(target):
        region_state = shaped[:, target]
        mean_state = lax.optimization_barrier(jnp.mean(region_state.astype(jnp.float32), axis=-1, keepdims=True))
        anomaly = (region_state - mean_state).astype(jnp.bfloat16)
        centre = jnp.dot(anomaly.reshape(-1, members), transform[target], preferred_element_type=jnp.float32)
        centre = centre.reshape(lag_count, HC, levels, members)
        western = jnp.dot(anomaly[:, :half_width].reshape(-1, members), preceding[target], preferred_element_type=jnp.float32)
        eastern = jnp.dot(anomaly[:, half_width:].reshape(-1, members), following[target], preferred_element_type=jnp.float32)
        beside = jnp.concatenate([western.reshape(lag_count, half_width, levels, members), eastern.reshape(lag_count, HC - half_width, levels, members)], axis=1)
        return (mean_state + (1.0 - blend_weight) * centre + blend_weight * beside).astype(jnp.bfloat16)
    updated = lax.map(region_update, jnp.arange(region_count, dtype=jnp.int32))
    return jnp.moveaxis(updated, 0, 1).reshape(states.shape)
```

```python
import functools

import jax
import jax.numpy as jnp
from jax import lax
from jax.experimental import pallas as pl
from jax.experimental.pallas import tpu as pltpu
from jax.sharding import PartitionSpec as P

HC = 32
NS_ITERS = 5
INFLATION = 1.1
HALO = 2
EXTRA = 16
MESH = pl.DeviceIdType.MESH
F32 = jnp.float32
BF16 = jnp.bfloat16
FWD, BWD, NEAR, FAR = range(4)


def iota2(shape, dim):
    return lax.broadcasted_iota(jnp.int32, shape, dim)


def pack(matrix, row):
    half = matrix.shape[0] // 2
    a, b, c = matrix[:half, :half], matrix[:half, half:], matrix[half:, half:]
    i, j = iota2((half, half), 0), iota2((half, half), 1)
    top = jnp.concatenate([b, jnp.where(j >= i, a, c)], axis=1)
    diagonal = jnp.sum(jnp.where(i == j, c, 0.0), axis=0, keepdims=True)
    second = jnp.concatenate([diagonal, jnp.zeros_like(diagonal)], axis=1)
    place = iota2((EXTRA, 2 * half), 0)
    extra = jnp.where(place == 0, row, jnp.where(place == 1, second, 0.0))
    return top, extra


def unpack(block):
    half = block.shape[0] - EXTRA
    b, d = block[:half, :half], block[:half, half:]
    row = block[half : half + 1]
    diagonal = block[half + 1 : half + 2, :half]
    i, j = iota2((half, half), 0), iota2((half, half), 1)
    flipped = d.T
    a = jnp.where(j >= i, d, flipped)
    c = jnp.where(i > j, d, jnp.where(i < j, flipped, diagonal))
    matrix = jnp.concatenate(
        [jnp.concatenate([a, b], axis=1), jnp.concatenate([b.T, c], axis=1)], axis=0
    )
    return matrix, row


def transform_parts(gram, vec):
    n = gram.shape[0]
    both = lambda x: jnp.sum(jnp.sum(x, axis=0, keepdims=True), axis=1, keepdims=True)
    identity = (iota2(gram.shape, 0) == iota2(gram.shape, 1)).astype(F32)
    system = gram + (n - 1) / INFLATION * identity
    frob = jnp.sqrt(both(system * system))
    inverse_frob = 1.0 / frob
    a = both(system * identity) * (1.0 / n) * inverse_frob
    rest = system * inverse_frob - a * identity
    u = jnp.broadcast_to(vec, (EXTRA, n))
    dot = functools.partial(jnp.dot, preferred_element_type=F32)
    z_one = z_rest = None
    for step in range(NS_ITERS):
        last = step == NS_ITERS - 1
        h = 1.5 - 0.5 * a
        r = rest.astype(BF16)
        left = [] if last else [r]
        if step:
            left.append(z_rest.astype(BF16))
        left.append(u.astype(BF16))
        first = dot(jnp.concatenate(left, axis=0), r)
        turned = h * u - 0.5 * first[-EXTRA:]
        if step:
            z_rest = h * z_rest - (0.5 * z_one) * rest - 0.5 * first[-EXTRA - n : -EXTRA]
            z_one = h * z_one
        else:
            z_rest, z_one = -0.5 * rest, h
        left = [] if last else [first[:n].astype(BF16)]
        left.append(turned.astype(BF16))
        second = dot(jnp.concatenate(left, axis=0), r)
        u = h * turned - 0.5 * second[-EXTRA:]
        if not last:
            rest = (
                (2.25 - 3.0 * a + 0.75 * a * a) * rest
                + (0.75 * a - 1.5) * first[:n]
                + 0.25 * second[:n]
            )
            a = a * h * h
    scale = jnp.sqrt(F32(n - 1.0)) * lax.rsqrt(frob)
    spread = (z_rest + z_one * identity) * scale
    return spread, u[0:1] * inverse_frob


def assimilate(
    n_space,
    count_hbm, radius_hbm, obs_hbm, innov_hbm, weight_hbm, column_hbm, states_hbm, out_ref,
    count_ref, radius_ref, innov_ref, weight_ref, column_ref, anomaly, means, tmat, obs_v, obs_t,
    mine, near_in, edge_out, halo_in, own, cross_out, cross_in, t_out, t_in,
    load_sem, small_sem, near_send, near_recv, edge_send, halo_recv, cross_send, cross_recv,
    t_send, t_recv,
):
    tm, sp = lax.axis_index("tm"), lax.axis_index("space")
    after, before = lax.rem(sp + 1, n_space), lax.rem(sp + n_space - 1, n_space)
    chip, core = tm // 2, lax.rem(tm, 2)
    partner, cross = 2 * chip + 1 - core, 2 * (1 - chip) + core
    regions, capacity, members = obs_v.shape
    half = members // 2
    region_of = lambda t: lax.rem(t + 2, 3) + t // 3
    low_owner, high_owner = 1, 3
    here = lambda t: {"tm": t, "space": sp}

    def remote(src, dst, send, recv, device):
        return pltpu.make_async_remote_copy(
            src_ref=src, dst_ref=dst, send_sem=send, recv_sem=recv, device_id=device, device_id_type=MESH
        )

    def arrived(ref, sem):
        pltpu.make_async_copy(ref, ref, sem).wait()

    loads = [
        pltpu.make_async_copy(obs_hbm.at[0, r], obs_v.at[r], load_sem.at[r]) for r in range(regions)
    ]
    small = [
        pltpu.make_async_copy(src, dst, small_sem.at[n])
        for n, (src, dst) in enumerate(
            [
                (count_hbm, count_ref),
                (radius_hbm, radius_ref),
                (innov_hbm.at[0], innov_ref),
                (weight_hbm.at[0], weight_ref),
                (column_hbm.at[0], column_ref),
                (states_hbm, anomaly),
            ]
        )
    ]
    for load in small[:-1] + loads[::-1] + small[-1:]:
        load.start()

    barrier = pltpu.get_barrier_semaphore()
    peers = [lax.rem(tm + d, 4) for d in range(1, 4)]
    greeted = [(p, sp) for p in peers]
    greeted += [(t, s) for s in (before, after) for t in range(4)]
    for t, s in greeted:
        pl.semaphore_signal(barrier, inc=1, device_id={"tm": t, "space": s}, device_id_type=MESH)

    for load in small[:-1]:
        load.wait()
    shape = (regions, capacity)
    which = iota2(shape, 0)
    count = jnp.zeros(shape, jnp.int32)
    radius = jnp.zeros(shape, jnp.int32)
    for r in range(regions):
        count = jnp.where(which == r, count_ref[0, r], count)
        radius = jnp.where(which == r, radius_ref[r], radius)
    present = (iota2(shape, 1) < count).astype(F32)
    base = weight_ref[...] * present
    inverse_radius = 1.0 / radius.astype(F32)
    position = column_ref[...].astype(F32) + 0.5 - 0.5 * HC
    weights, pulls = [], []
    for offset in range(-HALO, HALO + 1):
        ratio = jnp.minimum(jnp.abs(position - offset * HC) * inverse_radius, 1.0)
        weight = base * jnp.square(1.0 - ratio * ratio)
        weights.append(weight)
        pulls.append(weight * innov_ref[...])

    first_row = iota2((EXTRA, capacity), 0) == 0

    def gram_of(target):
        total = None
        for r in range(max(0, target - 2 * HALO), min(regions, target + 1)):
            k = target - r
            weight = jnp.broadcast_to(weights[k][r : r + 1], (16, capacity)).astype(BF16)
            pull = jnp.where(first_row, pulls[k][r : r + 1], 0.0).astype(BF16)
            scaled = obs_t[r].reshape(members // 16, 16, capacity) * weight[None]
            left = jnp.concatenate([scaled.reshape(members, capacity), pull], axis=0)
            part = jnp.dot(left, obs_v[r], preferred_element_type=F32)
            total = part if total is None else total + part
        top, extra = pack(total[:members], total[members : members + 1])
        mine[target, :half] = top.astype(BF16)
        mine[target, half:] = extra.astype(BF16)

    def near_copy(group, block):
        return remote(
            mine.at[block], near_in.at[group], near_send.at[group], near_recv.at[group], here(partner)
        )

    def chip_sum(group, block):
        arrived(near_in.at[group], near_recv.at[group])
        return mine[block].astype(F32) + near_in[group].astype(F32)

    def edge_copy(group, owner, space):
        edge_out[group] = chip_sum(group, own_block[group]).astype(BF16)
        return remote(
            edge_out.at[group],
            halo_in.at[chip],
            edge_send.at[group],
            halo_recv.at[chip],
            {"tm": owner, "space": space},
        )

    cross_copy = remote(cross_out, cross_in, cross_send, cross_recv, here(cross))

    def settle(group, keep):
        total = chip_sum(group, own_block[group])

        @pl.when(keep)
        def _():
            own[...] = total

        @pl.when(jnp.logical_not(keep))
        def _():
            cross_out[...] = total.astype(BF16)
            cross_copy.start()

    own_block = {FWD: 7 - core, BWD: core, FAR: 4 + core, NEAR: 3 - core}
    partner_block = {FWD: 6 + core, BWD: 1 - core, FAR: 5 - core, NEAR: 2 + core}
    near = {g: near_copy(g, partner_block[g]) for g in (FWD, FAR, NEAR, BWD)}

    with jax.named_scope("p1_fwd"):
        loads[3].wait()
        obs_t[3] = obs_v[3].T
        gram_of(7)
        loads[2].wait()
        obs_t[2] = obs_v[2].T
        gram_of(6)
    with jax.named_scope("p2_barrier"):
        pl.semaphore_wait(barrier, len(greeted))
    near[FWD].start()
    with jax.named_scope("p3_far"):
        for r in (1, 0):
            loads[r].wait()
            obs_t[r] = obs_v[r].T
        gram_of(5)
        gram_of(4)
    near[FAR].start()
    with jax.named_scope("p4_fwdsum"):
        edge_fwd = edge_copy(FWD, 2 - core, after)
    edge_fwd.start()
    with jax.named_scope("p5_near"):
        gram_of(3)
        gram_of(2)
    near[NEAR].start()
    with jax.named_scope("p6_farsum"):
        settle(FAR, chip == core)
    with jax.named_scope("p7_bwd"):
        gram_of(1)
        gram_of(0)
    near[BWD].start()
    with jax.named_scope("p8_nearsum"):
        settle(NEAR, chip != core)

    small[-1].wait()
    lags, _, rows, _ = anomaly.shape

    def centre_on_mean(n, carry):
        lag, r = n // regions, lax.rem(n, regions)
        x = anomaly[lag, r].astype(F32)
        mean = jnp.sum(x, axis=1, keepdims=True) * (1.0 / members)
        means[lag, r] = mean
        anomaly[lag, r] = (x - mean).astype(BF16)
        return carry

    with jax.named_scope("p9_bwdsum"):
        edge_bwd = edge_copy(BWD, 3 * core, before)
    edge_bwd.start()
    with jax.named_scope("q0_centre"):
        lax.fori_loop(0, lags * regions, centre_on_mean, 0)

    with jax.named_scope("q1_cross"):
        arrived(cross_in, cross_recv)
    with jax.named_scope("q2_halo"):
        for x in range(2):
            arrived(halo_in.at[x], halo_recv.at[x])
    with jax.named_scope("q3_ns"):
        total = own[...] + cross_in[...].astype(F32)
        gram, vec = unpack(total + (halo_in[0].astype(F32) + halo_in[1].astype(F32)))
        spread, wbar = transform_parts(gram, vec)
        top, extra = pack(spread, wbar)
        t_out[:half] = top.astype(BF16)
        t_out[half:] = extra.astype(BF16)

    own_slot, cross_slot = region_of(tm) + 1, region_of(cross) + 1
    near_slot, last_slot = region_of(partner) + 1, region_of(2 * (1 - chip) + 1 - core) + 1

    def send_transform(n, slot, device):
        return remote(t_out, t_in.at[slot], t_send.at[n], t_recv.at[slot], device)

    t_cross = send_transform(0, own_slot, here(cross))
    t_near = send_transform(1, own_slot, here(partner))
    order = [1, 0, 3, 2]
    high = [send_transform(2 + n, 0, {"tm": t, "space": after}) for n, t in enumerate(order)]
    low = [send_transform(2 + n, regions + 1, {"tm": t, "space": before}) for n, t in enumerate(order)]
    relay = remote(t_in.at[cross_slot], t_in.at[cross_slot], t_send.at[6], t_recv.at[cross_slot], here(partner))

    t_cross.start()

    @pl.when(tm == low_owner)
    def _():
        for copy in low:
            copy.start()

    @pl.when(tm == high_owner)
    def _():
        for copy in high:
            copy.start()

    t_near.start()

    def place(slot, block):
        matrix, row = unpack(block.astype(F32))
        tmat[slot] = (matrix + row).astype(BF16)

    def wait_slot(slot):
        arrived(t_in.at[slot], t_recv.at[slot])

    mid = rows // 2

    def update(r, side):
        part = slice(side * mid, (side + 1) * mid)
        column = (iota2((mid, 1), 0) + side * mid) // (rows // HC)
        blend = jnp.abs((column.astype(F32) + 0.5) / HC - 0.5)
        for lag in range(lags):
            block = anomaly[lag, r, part]

            def apply(slot):
                return lax.dot_general(
                    block, tmat[slot], (((1,), (1,)), ((), ())), preferred_element_type=F32
                )

            centre, beside = apply(r + 1), apply(r + 2 * side)
            mean = means[lag, r, part]
            out_ref[lag, r, part] = (mean + centre + blend * (beside - centre)).astype(BF16)

    with jax.named_scope("q4_place"):
        place(own_slot, t_out[...])
    with jax.named_scope("q5_near"):
        wait_slot(near_slot)
        place(near_slot, t_in[near_slot])
    with jax.named_scope("q6_cross"):
        wait_slot(cross_slot)
    relay.start()
    with jax.named_scope("q7_last"):
        place(cross_slot, t_in[cross_slot])
        wait_slot(last_slot)
        place(last_slot, t_in[last_slot])
    with jax.named_scope("q8_update"):
        for r in range(regions):
            for side in range(2):
                if (r, side) not in ((0, 0), (regions - 1, 1)):
                    update(r, side)
    with jax.named_scope("q9_wait4"):
        wait_slot(regions + 1)
    with jax.named_scope("r0_upd"):
        place(regions + 1, t_in[regions + 1])
        update(regions - 1, 1)
    with jax.named_scope("r1_wait0"):
        wait_slot(0)
    with jax.named_scope("r2_upd"):
        place(0, t_in[0])
        update(0, 0)

    with jax.named_scope("r3_drain"):
        for copy in (*near.values(), edge_fwd, edge_bwd, cross_copy, t_cross, t_near, relay):
            copy.wait_send()

        @pl.when(tm == low_owner)
        def _():
            for copy in low:
                copy.wait_send()

        @pl.when(tm == high_owner)
        def _():
            for copy in high:
                copy.wait_send()


def shards(n_tm, n_space, obs, innovation, error_weight, obs_column, obs_count, radius, states):
    _, regions, capacity, members = obs.shape
    assert regions == n_tm == 4 and obs.shape[0] == 1
    rows = members // 2 + EXTRA
    lags, columns, levels, _ = states.shape
    shaped = states.reshape(lags, regions, columns // regions * levels, members)
    hbm = pl.BlockSpec(memory_space=pltpu.HBM)
    dma = pltpu.SemaphoreType.DMA
    packed = (rows, members)
    result = pl.pallas_call(
        functools.partial(assimilate, n_space),
        out_shape=pltpu.VMEM(shaped.shape, BF16),
        in_specs=[hbm] * 7,
        out_specs=pl.BlockSpec(memory_space=pltpu.VMEM),
        scratch_shapes=[
            pltpu.SMEM(obs_count.shape, jnp.int32),
            pltpu.SMEM(radius.shape, jnp.int32),
            pltpu.VMEM((regions, capacity), F32),
            pltpu.VMEM((regions, capacity), F32),
            pltpu.VMEM((regions, capacity), jnp.int32),
            pltpu.VMEM(shaped.shape, BF16),
            pltpu.VMEM(shaped.shape[:-1] + (1,), F32),
            pltpu.VMEM((regions + 2, members, members), BF16),
            pltpu.VMEM((regions, capacity, members), BF16),
            pltpu.VMEM((regions, members, capacity), BF16),
            pltpu.VMEM((regions + 2 * HALO, *packed), BF16),
            pltpu.VMEM((4, *packed), BF16),
            pltpu.VMEM((2, *packed), BF16),
            pltpu.VMEM((2, *packed), BF16),
            pltpu.VMEM(packed, F32),
            pltpu.VMEM(packed, BF16),
            pltpu.VMEM(packed, BF16),
            pltpu.VMEM(packed, BF16),
            pltpu.VMEM((regions + 2, *packed), BF16),
            dma((regions,)),
            dma((6,)),
            dma((4,)),
            dma((4,)),
            dma((2,)),
            dma((2,)),
            dma,
            dma,
            dma((7,)),
            dma((regions + 2,)),
        ],
        compiler_params=pltpu.CompilerParams(
            collective_id=0, has_side_effects=True, vmem_limit_bytes=67043328 - 2228224
        ),
        name="assimilate",
    )(obs_count, radius, obs, innovation, error_weight, obs_column, shaped)
    return result.reshape(states.shape)


def solution(mesh):
    return jax.shard_map(
        functools.partial(shards, mesh.shape["tm"], mesh.shape["space"]),
        mesh=mesh,
        in_specs=(
            P("tm", "space", None, None),
            P("tm", "space", None),
            P("tm", "space", None),
            P("tm", "space", None),
            P("tm", "space"),
            P("space"),
            P("tm", "space", None, None),
        ),
        out_specs=P("tm", "space", None, None),
        check_vma=False,
    )
```

```python
import functools

import jax
import jax.numpy as jnp
from jax import lax
from jax.experimental import pallas as pl
from jax.experimental.pallas import tpu as pltpu
from jax.sharding import PartitionSpec as P

HC = 32
NS_ITERS = 5
INFLATION = 1.1
HALO = 2
EXTRA = 16
MESH = pl.DeviceIdType.MESH
F32 = jnp.float32
BF16 = jnp.bfloat16
FWD, BWD, NEAR, FAR = range(4)


def iota2(shape, dim):
    return lax.broadcasted_iota(jnp.int32, shape, dim)


def pack(matrix, row):
    half = matrix.shape[0] // 2
    a, b, c = matrix[:half, :half], matrix[:half, half:], matrix[half:, half:]
    i, j = iota2((half, half), 0), iota2((half, half), 1)
    top = jnp.concatenate([b, jnp.where(j >= i, a, c)], axis=1)
    diagonal = jnp.sum(jnp.where(i == j, c, 0.0), axis=0, keepdims=True)
    second = jnp.concatenate([diagonal, jnp.zeros_like(diagonal)], axis=1)
    place = iota2((EXTRA, 2 * half), 0)
    extra = jnp.where(place == 0, row, jnp.where(place == 1, second, 0.0))
    return top, extra


def unpack(block):
    half = block.shape[0] - EXTRA
    b, d = block[:half, :half], block[:half, half:]
    row = block[half : half + 1]
    diagonal = block[half + 1 : half + 2, :half]
    i, j = iota2((half, half), 0), iota2((half, half), 1)
    flipped = d.T
    a = jnp.where(j >= i, d, flipped)
    c = jnp.where(i > j, d, jnp.where(i < j, flipped, diagonal))
    matrix = jnp.concatenate(
        [jnp.concatenate([a, b], axis=1), jnp.concatenate([b.T, c], axis=1)], axis=0
    )
    return matrix, row


def transform_parts(gram, vec):
    n = gram.shape[0]
    both = lambda x: jnp.sum(jnp.sum(x, axis=0, keepdims=True), axis=1, keepdims=True)
    identity = (iota2(gram.shape, 0) == iota2(gram.shape, 1)).astype(F32)
    system = gram + (n - 1) / INFLATION * identity
    frob = jnp.sqrt(both(system * system))
    inverse_frob = 1.0 / frob
    a = both(system * identity) * (1.0 / n) * inverse_frob
    rest = system * inverse_frob - a * identity
    u = jnp.broadcast_to(vec, (EXTRA, n))
    dot = functools.partial(jnp.dot, preferred_element_type=F32)
    z_one = z_rest = None
    for step in range(NS_ITERS):
        last = step == NS_ITERS - 1
        h = 1.5 - 0.5 * a
        r = rest.astype(BF16)
        left = [] if last else [r]
        if step:
            left.append(z_rest.astype(BF16))
        left.append(u.astype(BF16))
        first = dot(jnp.concatenate(left, axis=0), r)
        turned = h * u - 0.5 * first[-EXTRA:]
        if step:
            z_rest = h * z_rest - (0.5 * z_one) * rest - 0.5 * first[-EXTRA - n : -EXTRA]
            z_one = h * z_one
        else:
            z_rest, z_one = -0.5 * rest, h
        left = [] if last else [first[:n].astype(BF16)]
        left.append(turned.astype(BF16))
        second = dot(jnp.concatenate(left, axis=0), r)
        u = h * turned - 0.5 * second[-EXTRA:]
        if not last:
            rest = (
                (2.25 - 3.0 * a + 0.75 * a * a) * rest
                + (0.75 * a - 1.5) * first[:n]
                + 0.25 * second[:n]
            )
            a = a * h * h
    scale = jnp.sqrt(F32(n - 1.0)) * lax.rsqrt(frob)
    spread = (z_rest + z_one * identity) * scale
    return spread, u[0:1] * inverse_frob


def assimilate(
    n_space,
    count_hbm, radius_hbm, obs_hbm, innov_hbm, weight_hbm, column_hbm, states_hbm, anomaly, means, tmat,
    count_ref, radius_ref, innov_ref, weight_ref, column_ref, obs_v, obs_t,
    mine, near_in, edge_out, halo_in, own, cross_out, cross_in, t_out, t_in,
    load_sem, small_sem, near_send, near_recv, edge_send, halo_recv, cross_send, cross_recv,
    t_send, t_recv,
):
    tm, sp = lax.axis_index("tm"), lax.axis_index("space")
    after, before = lax.rem(sp + 1, n_space), lax.rem(sp + n_space - 1, n_space)
    chip, core = tm // 2, lax.rem(tm, 2)
    partner, cross = 2 * chip + 1 - core, 2 * (1 - chip) + core
    regions, capacity, members = obs_v.shape
    half = members // 2
    region_of = lambda t: lax.rem(t + 2, 3) + t // 3
    low_owner, high_owner = 1, 3
    here = lambda t: {"tm": t, "space": sp}

    def remote(src, dst, send, recv, device):
        return pltpu.make_async_remote_copy(
            src_ref=src, dst_ref=dst, send_sem=send, recv_sem=recv, device_id=device, device_id_type=MESH
        )

    def arrived(ref, sem):
        pltpu.make_async_copy(ref, ref, sem).wait()

    loads = [
        pltpu.make_async_copy(obs_hbm.at[0, r], obs_v.at[r], load_sem.at[r]) for r in range(regions)
    ]
    small = [
        pltpu.make_async_copy(src, dst, small_sem.at[n])
        for n, (src, dst) in enumerate(
            [
                (count_hbm, count_ref),
                (radius_hbm, radius_ref),
                (innov_hbm.at[0], innov_ref),
                (weight_hbm.at[0], weight_ref),
                (column_hbm.at[0], column_ref),
                (states_hbm, anomaly),
            ]
        )
    ]
    for load in loads[-1:] + small[:-1] + loads[-2::-1] + small[-1:]:
        load.start()

    barrier = pltpu.get_barrier_semaphore()
    peers = [lax.rem(tm + d, 4) for d in range(1, 4)]
    greeted = [(p, sp) for p in peers]
    greeted += [(t, s) for s in (before, after) for t in range(4)]
    for t, s in greeted:
        pl.semaphore_signal(barrier, inc=1, device_id={"tm": t, "space": s}, device_id_type=MESH)

    def turn(r):
        loads[r].wait()
        obs_t[r] = obs_v[r].T

    for load in small[:-1]:
        load.wait()
    turn(regions - 1)
    shape = (regions, capacity)
    which = iota2(shape, 0)
    count = jnp.zeros(shape, jnp.int32)
    radius = jnp.zeros(shape, jnp.int32)
    for r in range(regions):
        count = jnp.where(which == r, count_ref[0, r], count)
        radius = jnp.where(which == r, radius_ref[r], radius)
    present = (iota2(shape, 1) < count).astype(F32)
    base = weight_ref[...] * present
    inverse_radius = 1.0 / radius.astype(F32)
    position = column_ref[...].astype(F32) + 0.5 - 0.5 * HC
    weights, pulls = [], []
    for offset in range(-HALO, HALO + 1):
        ratio = jnp.minimum(jnp.abs(position - offset * HC) * inverse_radius, 1.0)
        weight = base * jnp.square(1.0 - ratio * ratio)
        weights.append(weight)
        pulls.append(weight * innov_ref[...])

    first_row = iota2((EXTRA, capacity), 0) == 0

    def gram_of(target):
        total = None
        for r in range(max(0, target - 2 * HALO), min(regions, target + 1)):
            k = target - r
            weight = jnp.broadcast_to(weights[k][r : r + 1], (16, capacity)).astype(BF16)
            pull = jnp.where(first_row, pulls[k][r : r + 1], 0.0).astype(BF16)
            scaled = obs_t[r].reshape(members // 16, 16, capacity) * weight[None]
            left = jnp.concatenate([scaled.reshape(members, capacity), pull], axis=0)
            part = jnp.dot(left, obs_v[r], preferred_element_type=F32)
            total = part if total is None else total + part
        top, extra = pack(total[:members], total[members : members + 1])
        mine[target, :half] = top.astype(BF16)
        mine[target, half:] = extra.astype(BF16)

    def near_copy(group, block):
        return remote(
            mine.at[block], near_in.at[group], near_send.at[group], near_recv.at[group], here(partner)
        )

    def chip_sum(group, block):
        arrived(near_in.at[group], near_recv.at[group])
        return mine[block].astype(F32) + near_in[group].astype(F32)

    def edge_copy(group, owner, space):
        return remote(
            edge_out.at[group],
            halo_in.at[chip],
            edge_send.at[group],
            halo_recv.at[chip],
            {"tm": owner, "space": space},
        )

    edges = {FWD: edge_copy(FWD, 2 - core, after), BWD: edge_copy(BWD, 3 * core, before)}

    def send_edge(group):
        edge_out[group] = chip_sum(group, own_block[group]).astype(BF16)
        edges[group].start()

    cross_copy = remote(cross_out, cross_in, cross_send, cross_recv, here(cross))

    def settle(group):
        total = chip_sum(group, own_block[group])
        keep = chip == (core if group == FAR else 1 - core)

        @pl.when(keep)
        def _():
            own[...] = total

        @pl.when(jnp.logical_not(keep))
        def _():
            cross_out[...] = total.astype(BF16)
            cross_copy.start()

    own_block = {FWD: 7 - core, BWD: core, FAR: 4 + core, NEAR: 3 - core}
    partner_block = {FWD: 6 + core, BWD: 1 - core, FAR: 5 - core, NEAR: 2 + core}
    near = {g: near_copy(g, partner_block[g]) for g in (FWD, FAR, NEAR, BWD)}

    with jax.named_scope("p1_fwd"):
        gram_of(7)
        turn(2)
        gram_of(6)

    @pl.when(sp == 0)
    def _():
        turn(1)
        turn(0)
        for target in range(5, -1, -1):
            gram_of(target)

    with jax.named_scope("p2_barrier"):
        pl.semaphore_wait(barrier, len(greeted))

    @pl.when(sp == 0)
    def _():
        for group in (BWD, FAR, NEAR, FWD):
            near[group].start()
        send_edge(BWD)
        settle(FAR)
        settle(NEAR)
        send_edge(FWD)

    @pl.when(sp != 0)
    def _():
        near[FWD].start()
        with jax.named_scope("p3_bwd"):
            turn(1)
            turn(0)
            gram_of(1)
            gram_of(0)
        near[BWD].start()
        with jax.named_scope("p4_five"):
            gram_of(5)
        with jax.named_scope("p5_fwdsum"):
            send_edge(FWD)
        with jax.named_scope("p6_four"):
            gram_of(4)
        near[FAR].start()
        with jax.named_scope("p7_bwdsum"):
            send_edge(BWD)
        with jax.named_scope("p8_near"):
            gram_of(3)
            gram_of(2)
        near[NEAR].start()
        with jax.named_scope("p9_sums"):
            settle(FAR)
            settle(NEAR)

    small[-1].wait()
    lags = anomaly.shape[0]

    def centre_on_mean(n, carry):
        lag, r = n // regions, lax.rem(n, regions)
        x = anomaly[lag, r].astype(F32)
        mean = jnp.sum(x, axis=1, keepdims=True) * (1.0 / members)
        means[lag, r] = mean
        anomaly[lag, r] = (x - mean).astype(BF16)
        return carry

    with jax.named_scope("q0_centre"):
        lax.fori_loop(0, lags * regions, centre_on_mean, 0)

    with jax.named_scope("q1_cross"):
        arrived(cross_in, cross_recv)
    with jax.named_scope("q2_halo"):
        for x in range(2):
            arrived(halo_in.at[x], halo_recv.at[x])
    with jax.named_scope("q3_ns"):
        total = own[...] + cross_in[...].astype(F32)
        gram, vec = unpack(total + (halo_in[0].astype(F32) + halo_in[1].astype(F32)))
        spread, wbar = transform_parts(gram, vec)
        top, extra = pack(spread, wbar)
        t_out[:half] = top.astype(BF16)
        t_out[half:] = extra.astype(BF16)

    own_slot, cross_slot = region_of(tm) + 1, region_of(cross) + 1
    near_slot, last_slot = region_of(partner) + 1, region_of(2 * (1 - chip) + 1 - core) + 1

    def send_transform(n, slot, device):
        return remote(t_out, t_in.at[slot], t_send.at[n], t_recv.at[slot], device)

    t_cross = send_transform(0, own_slot, here(cross))
    t_near = send_transform(1, own_slot, here(partner))
    to_high = lambda n, t: send_transform(2 + n, 0, {"tm": t, "space": after})
    to_low = lambda n, t: send_transform(2 + n, regions + 1, {"tm": t, "space": before})
    high = [to_high(n, t) for n, t in enumerate((3, 2, 1, 0))]
    low = [to_low(n, t) for n, t in enumerate((1, 0, 3, 2))]
    end = sp == n_space - 1
    relay = remote(t_in.at[cross_slot], t_in.at[cross_slot], t_send.at[6], t_recv.at[cross_slot], here(partner))

    @pl.when(jnp.logical_and(tm == high_owner, end))
    def _():
        for n in (3, 2, 0, 1):
            high[n].start()

    t_cross.start()
    t_near.start()

    @pl.when(tm == low_owner)
    def _():
        for copy in low:
            copy.start()

    @pl.when(jnp.logical_and(tm == high_owner, jnp.logical_not(end)))
    def _():
        for copy in high:
            copy.start()

    def place(slot, block):
        matrix, row = unpack(block.astype(F32))
        tmat[slot] = (matrix + row).astype(BF16)

    def wait_slot(slot):
        arrived(t_in.at[slot], t_recv.at[slot])

    with jax.named_scope("q4_place"):
        place(own_slot, t_out[...])
    with jax.named_scope("q5_near"):
        wait_slot(near_slot)
        place(near_slot, t_in[near_slot])
    with jax.named_scope("q6_cross"):
        wait_slot(cross_slot)
    relay.start()
    with jax.named_scope("q7_last"):
        place(cross_slot, t_in[cross_slot])
        wait_slot(last_slot)
        place(last_slot, t_in[last_slot])
    with jax.named_scope("q8_above"):
        wait_slot(regions + 1)
        place(regions + 1, t_in[regions + 1])
    with jax.named_scope("q9_below"):
        wait_slot(0)
        place(0, t_in[0])

    with jax.named_scope("r3_drain"):
        for copy in (*near.values(), *edges.values(), cross_copy, t_cross, t_near, relay):
            copy.wait_send()

        @pl.when(tm == low_owner)
        def _():
            for copy in low:
                copy.wait_send()

        @pl.when(tm == high_owner)
        def _():
            for copy in high:
                copy.wait_send()


def finish(anomaly, means, tmat, out_hbm, staged, sems):
    lags, regions, rows, _ = anomaly.shape
    mid = rows // 2
    copies = []
    for r in range(regions):
        for side in range(2):
            part = slice(side * mid, (side + 1) * mid)
            column = (iota2((mid, 1), 0) + side * mid) // (rows // HC)
            blend = jnp.abs((column.astype(F32) + 0.5) / HC - 0.5)
            for lag in range(lags):
                block = anomaly[lag, r, part]

                def apply(slot):
                    return lax.dot_general(
                        block, tmat[slot], (((1,), (1,)), ((), ())), preferred_element_type=F32
                    )

                centre, beside = apply(r + 1), apply(r + 2 * side)
                mean = means[lag, r, part]
                staged[lag, r, part] = (mean + centre + blend * (beside - centre)).astype(BF16)
                copies.append(
                    pltpu.make_async_copy(
                        staged.at[lag, r, part], out_hbm.at[lag, r, part], sems.at[lag, r, side]
                    )
                )
                copies[-1].start()
    for copy in copies:
        copy.wait()


def shards(n_tm, n_space, obs, innovation, error_weight, obs_column, obs_count, radius, states):
    _, regions, capacity, members = obs.shape
    assert regions == n_tm == 4 and obs.shape[0] == 1
    rows = members // 2 + EXTRA
    lags, columns, levels, _ = states.shape
    shaped = states.reshape(lags, regions, columns // regions * levels, members)
    hbm = pl.BlockSpec(memory_space=pltpu.HBM)
    dma = pltpu.SemaphoreType.DMA
    packed = (rows, members)
    vmem = pl.BlockSpec(memory_space=pltpu.VMEM)
    parts = pl.pallas_call(
        functools.partial(assimilate, n_space),
        out_shape=[
            pltpu.VMEM(shaped.shape, BF16),
            pltpu.VMEM(shaped.shape[:-1] + (1,), F32),
            pltpu.VMEM((regions + 2, members, members), BF16),
        ],
        in_specs=[hbm] * 7,
        out_specs=[vmem] * 3,
        scratch_shapes=[
            pltpu.SMEM(obs_count.shape, jnp.int32),
            pltpu.SMEM(radius.shape, jnp.int32),
            pltpu.VMEM((regions, capacity), F32),
            pltpu.VMEM((regions, capacity), F32),
            pltpu.VMEM((regions, capacity), jnp.int32),
            pltpu.VMEM((regions, capacity, members), BF16),
            pltpu.VMEM((regions, members, capacity), BF16),
            pltpu.VMEM((regions + 2 * HALO, *packed), BF16),
            pltpu.VMEM((4, *packed), BF16),
            pltpu.VMEM((2, *packed), BF16),
            pltpu.VMEM((2, *packed), BF16),
            pltpu.VMEM(packed, F32),
            pltpu.VMEM(packed, BF16),
            pltpu.VMEM(packed, BF16),
            pltpu.VMEM(packed, BF16),
            pltpu.VMEM((regions + 2, *packed), BF16),
            dma((regions,)),
            dma((6,)),
            dma((4,)),
            dma((4,)),
            dma((2,)),
            dma((2,)),
            dma,
            dma,
            dma((7,)),
            dma((regions + 2,)),
        ],
        compiler_params=pltpu.CompilerParams(
            collective_id=0, has_side_effects=True, vmem_limit_bytes=67043328 - 5111808
        ),
        name="assimilate",
    )(obs_count, radius, obs, innovation, error_weight, obs_column, shaped)
    result = pl.pallas_call(
        finish,
        out_shape=jax.ShapeDtypeStruct(shaped.shape, BF16),
        in_specs=[vmem] * 3,
        out_specs=hbm,
        scratch_shapes=[pltpu.VMEM(shaped.shape, BF16), dma((lags, regions, 2))],
        compiler_params=pltpu.CompilerParams(vmem_limit_bytes=32 << 20),
        name="finish",
    )(*parts)
    return result.reshape(states.shape)


def solution(mesh):
    return jax.shard_map(
        functools.partial(shards, mesh.shape["tm"], mesh.shape["space"]),
        mesh=mesh,
        in_specs=(
            P("tm", "space", None, None),
            P("tm", "space", None),
            P("tm", "space", None),
            P("tm", "space", None),
            P("tm", "space"),
            P("space"),
            P("tm", "space", None, None),
        ),
        out_specs=P("tm", "space", None, None),
        check_vma=False,
    )
```

```python
import functools

import jax
import jax.numpy as jnp
from jax import lax
from jax.experimental import pallas as pl
from jax.experimental.pallas import tpu as pltpu
from jax.sharding import PartitionSpec as P

HC = 32
NS_ITERS = 5
INFLATION = 1.1
HALO = 2
EXTRA = 16
MESH = pl.DeviceIdType.MESH
F32 = jnp.float32
BF16 = jnp.bfloat16
FWD, BWD, NEAR, FAR = range(4)


def iota2(shape, dim):
    return lax.broadcasted_iota(jnp.int32, shape, dim)


def pack(matrix, row):
    half = matrix.shape[0] // 2
    a, b, c = matrix[:half, :half], matrix[:half, half:], matrix[half:, half:]
    i, j = iota2((half, half), 0), iota2((half, half), 1)
    top = jnp.concatenate([b, jnp.where(j >= i, a, c)], axis=1)
    diagonal = jnp.sum(jnp.where(i == j, c, 0.0), axis=0, keepdims=True)
    second = jnp.concatenate([diagonal, jnp.zeros_like(diagonal)], axis=1)
    place = iota2((EXTRA, 2 * half), 0)
    extra = jnp.where(place == 0, row, jnp.where(place == 1, second, 0.0))
    return top, extra


def unpack(block):
    half = block.shape[0] - EXTRA
    b, d = block[:half, :half], block[:half, half:]
    row = block[half : half + 1]
    diagonal = block[half + 1 : half + 2, :half]
    i, j = iota2((half, half), 0), iota2((half, half), 1)
    flipped = d.T
    a = jnp.where(j >= i, d, flipped)
    c = jnp.where(i > j, d, jnp.where(i < j, flipped, diagonal))
    matrix = jnp.concatenate(
        [jnp.concatenate([a, b], axis=1), jnp.concatenate([b.T, c], axis=1)], axis=0
    )
    return matrix, row


def transform_parts(gram, vec, shift):
    n = gram.shape[0]
    both = lambda x: jnp.sum(jnp.sum(x, axis=0, keepdims=True), axis=1, keepdims=True)
    identity = (iota2(gram.shape, 0) == iota2(gram.shape, 1)).astype(F32)
    base = (n - 1) / INFLATION
    rest = gram - shift * identity
    r = rest.astype(BF16)
    u = jnp.broadcast_to(vec, (EXTRA, n))
    dot = functools.partial(jnp.dot, preferred_element_type=F32)
    first = dot(jnp.concatenate([r, u.astype(BF16)], axis=0), r)
    system = gram + base * identity
    frob = jnp.sqrt(both(system * system))
    unit = 1.0 / frob
    a = (shift + base) * unit
    h = 1.5 - 0.5 * a
    turned = h * u - (0.5 * unit) * first[n:]
    second = dot(jnp.concatenate([first[:n].astype(BF16), turned.astype(BF16)], axis=0), r)
    u = h * turned - (0.5 * unit) * second[n:]
    z_rest, z_one = (-0.5 * unit) * rest, h
    rest = (
        ((2.25 - 3.0 * a + 0.75 * a * a) * unit) * rest
        + ((0.75 * a - 1.5) * unit * unit) * first[:n]
        + (0.25 * unit * unit * unit) * second[:n]
    )
    a = a * h * h
    for step in range(1, NS_ITERS):
        last = step == NS_ITERS - 1
        h = 1.5 - 0.5 * a
        r = rest.astype(BF16)
        left = [z_rest.astype(BF16), u.astype(BF16)]
        first = dot(jnp.concatenate(left if last else [r, *left], axis=0), r)
        turned = h * u - 0.5 * first[-EXTRA:]
        z_rest = h * z_rest - (0.5 * z_one) * rest - 0.5 * first[-EXTRA - n : -EXTRA]
        z_one = h * z_one
        left = [] if last else [first[:n].astype(BF16)]
        left.append(turned.astype(BF16))
        second = dot(jnp.concatenate(left, axis=0), r)
        u = h * turned - 0.5 * second[-EXTRA:]
        if not last:
            rest = (
                (2.25 - 3.0 * a + 0.75 * a * a) * rest
                + (0.75 * a - 1.5) * first[:n]
                + 0.25 * second[:n]
            )
            a = a * h * h
    scale = jnp.sqrt(F32(n - 1.0)) * lax.rsqrt(frob)
    spread = (z_rest + z_one * identity) * scale
    return spread, u[0:1] * unit


def blended(block, mean, centre, beside, side):
    mid = block.shape[0]
    column = (iota2((mid, 1), 0) + side * mid) // (2 * mid // HC)
    blend = jnp.abs((column.astype(F32) + 0.5) / HC - 0.5)
    apply = lambda t: lax.dot_general(
        block, t, (((1,), (1,)), ((), ())), preferred_element_type=F32
    )
    own, other = apply(centre), apply(beside)
    return (mean + own + blend * (other - own)).astype(BF16)


def assimilate(
    n_space,
    count_hbm, radius_hbm, obs_hbm, innov_hbm, weight_hbm, column_hbm, states_hbm, done, anomaly, means, tmat,
    count_ref, radius_ref, innov_ref, weight_ref, column_ref, obs_v, obs_t,
    mine, near_in, edge_out, halo_in, own, cross_out, cross_in, t_out, t_in,
    load_sem, small_sem, near_send, near_recv, edge_send, halo_recv, cross_send, cross_recv,
    t_send, t_recv,
):
    tm, sp = lax.axis_index("tm"), lax.axis_index("space")
    after, before = lax.rem(sp + 1, n_space), lax.rem(sp + n_space - 1, n_space)
    chip, core = tm // 2, lax.rem(tm, 2)
    partner, cross = 2 * chip + 1 - core, 2 * (1 - chip) + core
    regions, capacity, members = obs_v.shape
    half = members // 2
    region_of = lambda x, c: (1 - x) * (1 - c) + x * (2 + c)
    here = lambda t: {"tm": t, "space": sp}

    def remote(src, dst, send, recv, device):
        return pltpu.make_async_remote_copy(
            src_ref=src, dst_ref=dst, send_sem=send, recv_sem=recv, device_id=device, device_id_type=MESH
        )

    def arrived(ref, sem):
        pltpu.make_async_copy(ref, ref, sem).wait()

    barrier = pltpu.get_barrier_semaphore()
    first, end = sp == 0, sp == n_space - 1
    low_owner, high_owner = 1, 3
    greet = lambda t, s: pl.semaphore_signal(
        barrier, inc=1, device_id={"tm": t, "space": s}, device_id_type=MESH
    )
    sender_space = jnp.where(chip == 0, before, after)
    greet(partner, sp)
    greet(cross, sp)
    greet(core, sender_space)
    greet(core + 2, sender_space)

    @pl.when(jnp.logical_and(first, tm == 0))
    def _():
        greet(high_owner, before)

    loads = [
        pltpu.make_async_copy(obs_hbm.at[0, r], obs_v.at[r], load_sem.at[r]) for r in range(regions)
    ]
    small = [
        pltpu.make_async_copy(src, dst, small_sem.at[n])
        for n, (src, dst) in enumerate(
            [
                (count_hbm, count_ref),
                (radius_hbm, radius_ref),
                (innov_hbm.at[0], innov_ref),
                (weight_hbm.at[0], weight_ref),
                (column_hbm.at[0], column_ref),
                (states_hbm, anomaly),
            ]
        )
    ]
    for load in loads[-1:] + small[:-1] + loads[-2::-1] + small[-1:]:
        load.start()

    def turn(r):
        loads[r].wait()
        obs_t[r] = obs_v[r].T

    for load in small[:-1]:
        load.wait()
    turn(regions - 1)
    shape = (regions, capacity)
    which = iota2(shape, 0)
    count = jnp.zeros(shape, jnp.int32)
    radius = jnp.zeros(shape, jnp.int32)
    for r in range(regions):
        count = jnp.where(which == r, count_ref[0, r], count)
        radius = jnp.where(which == r, radius_ref[r], radius)
    present = (iota2(shape, 1) < count).astype(F32)
    base = weight_ref[...] * present
    inverse_radius = 1.0 / radius.astype(F32)
    position = column_ref[...].astype(F32) + 0.5 - 0.5 * HC
    weights, pulls = [], []
    for offset in range(-HALO, HALO + 1):
        ratio = jnp.minimum(jnp.abs(position - offset * HC) * inverse_radius, 1.0)
        weight = base * jnp.square(1.0 - ratio * ratio)
        weights.append(weight)
        pulls.append(weight * innov_ref[...])

    first_row = iota2((EXTRA, capacity), 0) == 0

    def gram_of(target):
        total = None
        for r in range(max(0, target - 2 * HALO), min(regions, target + 1)):
            k = target - r
            weight = jnp.broadcast_to(weights[k][r : r + 1], (16, capacity)).astype(BF16)
            pull = jnp.where(first_row, pulls[k][r : r + 1], 0.0).astype(BF16)
            scaled = obs_t[r].reshape(members // 16, 16, capacity) * weight[None]
            left = jnp.concatenate([scaled.reshape(members, capacity), pull], axis=0)
            part = jnp.dot(left, obs_v[r], preferred_element_type=F32)
            total = part if total is None else total + part
        top, extra = pack(total[:members], total[members : members + 1])
        mine[target, :half] = top.astype(BF16)
        mine[target, half:] = extra.astype(BF16)

    def near_copy(group, block):
        return remote(
            mine.at[block], near_in.at[group], near_send.at[group], near_recv.at[group], here(partner)
        )

    def chip_sum(group, block):
        arrived(near_in.at[group], near_recv.at[group])
        return mine[block].astype(F32) + near_in[group].astype(F32)

    def edge_copy(group, owner, space):
        return remote(
            edge_out.at[group],
            halo_in.at[chip],
            edge_send.at[group],
            halo_recv.at[chip],
            {"tm": owner, "space": space},
        )

    edges = {FWD: edge_copy(FWD, core, after), BWD: edge_copy(BWD, 2 + core, before)}

    def send_edge(group):
        edge_out[group] = chip_sum(group, own_block[group]).astype(BF16)
        edges[group].start()

    cross_copy = remote(cross_out, cross_in, cross_send, cross_recv, here(cross))

    def settle(group):
        total = chip_sum(group, own_block[group])
        keep = chip == (1 if group == FAR else 0)

        @pl.when(keep)
        def _():
            own[...] = total

        @pl.when(jnp.logical_not(keep))
        def _():
            cross_out[...] = total.astype(BF16)
            cross_copy.start()

    own_block = {FWD: 7 - core, BWD: core, FAR: 4 + core, NEAR: 3 - core}
    partner_block = {FWD: 6 + core, BWD: 1 - core, FAR: 5 - core, NEAR: 2 + core}
    near = {g: near_copy(g, partner_block[g]) for g in (FWD, FAR, NEAR, BWD)}

    with jax.named_scope("p1_fwd"):
        gram_of(7)
        turn(2)
        gram_of(6)

    @pl.when(first)
    def _():
        turn(1)
        turn(0)
        for target in range(5, -1, -1):
            gram_of(target)

    with jax.named_scope("p2_barrier"):
        pl.semaphore_wait(barrier, jnp.where(jnp.logical_and(end, tm == high_owner), 5, 4))


    @pl.when(first)
    def _():
        for group in (BWD, FAR, NEAR, FWD):
            near[group].start()

        @pl.when(core == 1)
        def _():
            send_edge(BWD)

        settle(FAR)
        settle(NEAR)
        send_edge(FWD)

    @pl.when(jnp.logical_not(first))
    def _():
        near[FWD].start()
        with jax.named_scope("p3_bwd"):
            turn(1)
            turn(0)
            gram_of(1)
            gram_of(0)
        near[BWD].start()
        with jax.named_scope("p4_fwdsum"):
            send_edge(FWD)
        with jax.named_scope("p5_far"):
            gram_of(5)
            gram_of(4)
        near[FAR].start()
        with jax.named_scope("p6_bwdsum"):
            send_edge(BWD)
        with jax.named_scope("p7_near"):
            gram_of(3)
            gram_of(2)
        near[NEAR].start()
        with jax.named_scope("p8_farsum"):
            settle(FAR)
        with jax.named_scope("p9_nearsum"):
            settle(NEAR)

    small[-1].wait()
    lags, _, rows, _ = anomaly.shape
    mid = rows // 2

    def centre_on_mean(n, carry):
        lag, r = n // regions, lax.rem(n, regions)
        x = anomaly[lag, r].astype(F32)
        mean = jnp.sum(x, axis=1, keepdims=True) * (1.0 / members)
        means[lag, r] = mean
        anomaly[lag, r] = (x - mean).astype(BF16)
        return carry

    with jax.named_scope("q0_centre"):
        lax.fori_loop(0, lags * regions, centre_on_mean, 0)

    @pl.when(jnp.logical_and(first, core == 0))
    def _():
        send_edge(BWD)

    with jax.named_scope("q1_cross"):
        arrived(cross_in, cross_recv)
        total = own[...] + cross_in[...].astype(F32)
        corner, extra = total[:half, half:], total[half + 1 : half + 2, :half]
        corner = jnp.where(iota2((half, half), 0) == iota2((half, half), 1), corner, 0.0)
        diagonal = jnp.sum(corner, axis=0, keepdims=True) + extra
        shift = jnp.sum(diagonal, axis=1, keepdims=True) * (1.0 / members)
    with jax.named_scope("q2_halo"):
        for x in range(2):
            arrived(halo_in.at[x], halo_recv.at[x])
    with jax.named_scope("q3_ns"):
        gram, vec = unpack(total + (halo_in[0].astype(F32) + halo_in[1].astype(F32)))
        spread, wbar = transform_parts(gram, vec, shift)
        top, extra = pack(spread, wbar)
        t_out[:half] = top.astype(BF16)
        t_out[half:] = extra.astype(BF16)

    own_slot, cross_slot = region_of(chip, core) + 1, region_of(1 - chip, core) + 1
    near_slot, last_slot = region_of(chip, 1 - core) + 1, region_of(1 - chip, 1 - core) + 1

    def send_transform(n, slot, device):
        return remote(t_out, t_in.at[slot], t_send.at[n], t_recv.at[slot], device)

    t_cross = send_transform(0, own_slot, here(cross))
    t_near = send_transform(1, own_slot, here(partner))
    to_high = lambda n, t: send_transform(2 + n, 0, {"tm": t, "space": after})
    to_low = lambda n, t: send_transform(2 + n, regions + 1, {"tm": t, "space": before})
    high = [to_high(n, t) for n, t in enumerate((3, 1))]
    far_end = to_high(2, 0)
    low = [to_low(n, t) for n, t in enumerate((1, 3))]
    pass_on = lambda n, slot: remote(
        t_in.at[slot], t_in.at[slot], t_send.at[n], t_recv.at[slot], here(partner)
    )
    relay, relay_above, relay_below = pass_on(6, cross_slot), pass_on(7, regions + 1), pass_on(8, 0)
    served = jnp.logical_and(first, chip == 0)
    is_low, is_high = tm == low_owner, tm == high_owner

    @pl.when(jnp.logical_and(is_high, end))
    def _():
        for copy in (far_end, high[1], high[0]):
            copy.start()

    t_cross.start()
    t_near.start()

    @pl.when(is_low)
    def _():
        for copy in low:
            copy.start()

    @pl.when(jnp.logical_and(is_high, jnp.logical_not(end)))
    def _():
        for copy in high:
            copy.start()

    def place(slot, block):
        matrix, row = unpack(block.astype(F32))
        tmat[slot] = (matrix + row).astype(BF16)

    def wait_slot(slot):
        arrived(t_in.at[slot], t_recv.at[slot])

    with jax.named_scope("q4_place"):
        place(own_slot, t_out[...])
    with jax.named_scope("q5_near"):
        wait_slot(near_slot)
        place(near_slot, t_in[near_slot])
    def boundary(b):
        for lag in range(lags):
            for r, side in ((b, 1), (b + 1, 0)):
                part = slice(side * mid, (side + 1) * mid)
                done[lag, r, part] = blended(
                    anomaly[lag, r, part], means[lag, r, part], tmat[r + 1], tmat[r + 2 * side], side
                )

    with jax.named_scope("q6_bound1"):
        boundary(2 * chip)
    with jax.named_scope("q7_cross"):
        wait_slot(cross_slot)
        relay.start()
        place(cross_slot, t_in[cross_slot])

    @pl.when(core == 1)
    def _():
        with jax.named_scope("q8_relays"):
            wait_slot(regions + 1)
            relay_above.start()

            @pl.when(jnp.logical_not(served))
            def _():
                wait_slot(0)
                relay_below.start()

    with jax.named_scope("q8_bound2"):

        @pl.when(core == 0)
        def _():
            boundary(1)

    with jax.named_scope("q9_last"):
        wait_slot(last_slot)
        place(last_slot, t_in[last_slot])
    with jax.named_scope("r0_bound3"):

        @pl.when(core == 1)
        def _():
            boundary(1)

        boundary(2 - 2 * chip)

    with jax.named_scope("r1_above"):

        @pl.when(core == 0)
        def _():
            wait_slot(regions + 1)

        place(regions + 1, t_in[regions + 1])
    with jax.named_scope("r2_below"):

        @pl.when(jnp.logical_or(core == 0, served))
        def _():
            wait_slot(0)

        place(0, t_in[0])

    with jax.named_scope("r3_drain"):
        for copy in (*near.values(), *edges.values(), cross_copy, t_cross, t_near, relay):
            copy.wait_send()

        @pl.when(core == 1)
        def _():
            relay_above.wait_send()

            @pl.when(jnp.logical_not(served))
            def _():
                relay_below.wait_send()

        @pl.when(is_low)
        def _():
            for copy in low:
                copy.wait_send()

        @pl.when(is_high)
        def _():
            for copy in high:
                copy.wait_send()

            @pl.when(end)
            def _():
                far_end.wait_send()


def finish(done, anomaly, means, tmat, out_hbm, outer, sems):
    lags, regions, rows, _ = anomaly.shape
    mid = rows // 2
    copies = []

    def put(src, lag, r, side):
        dst = out_hbm.at[lag, r, slice(side * mid, (side + 1) * mid)]
        copies.append(pltpu.make_async_copy(src, dst, sems.at[lag, r, side]))
        copies[-1].start()

    ends = ((0, 0), (regions - 1, 1))
    for lag in range(lags):
        for r in range(regions):
            for side in range(2):
                if (r, side) not in ends:
                    put(done.at[lag, r, slice(side * mid, (side + 1) * mid)], lag, r, side)
    for r, side in ends:
        part = slice(side * mid, (side + 1) * mid)
        for lag in range(lags):
            outer[lag, side] = blended(
                anomaly[lag, r, part], means[lag, r, part], tmat[r + 1], tmat[r + 2 * side], side
            )
            put(outer.at[lag, side], lag, r, side)
    for copy in copies:
        copy.wait()


def shards(n_tm, n_space, obs, innovation, error_weight, obs_column, obs_count, radius, states):
    _, regions, capacity, members = obs.shape
    assert regions == n_tm == 4 and obs.shape[0] == 1
    rows = members // 2 + EXTRA
    lags, columns, levels, _ = states.shape
    shaped = states.reshape(lags, regions, columns // regions * levels, members)
    hbm = pl.BlockSpec(memory_space=pltpu.HBM)
    dma = pltpu.SemaphoreType.DMA
    packed = (rows, members)
    vmem = pl.BlockSpec(memory_space=pltpu.VMEM)
    parts = pl.pallas_call(
        functools.partial(assimilate, n_space),
        out_shape=[
            pltpu.VMEM(shaped.shape, BF16),
            pltpu.VMEM(shaped.shape, BF16),
            pltpu.VMEM(shaped.shape[:-1] + (1,), F32),
            pltpu.VMEM((regions + 2, members, members), BF16),
        ],
        in_specs=[hbm] * 7,
        out_specs=[vmem] * 4,
        scratch_shapes=[
            pltpu.SMEM(obs_count.shape, jnp.int32),
            pltpu.SMEM(radius.shape, jnp.int32),
            pltpu.VMEM((regions, capacity), F32),
            pltpu.VMEM((regions, capacity), F32),
            pltpu.VMEM((regions, capacity), jnp.int32),
            pltpu.VMEM((regions, capacity, members), BF16),
            pltpu.VMEM((regions, members, capacity), BF16),
            pltpu.VMEM((regions + 2 * HALO, *packed), BF16),
            pltpu.VMEM((4, *packed), BF16),
            pltpu.VMEM((2, *packed), BF16),
            pltpu.VMEM((2, *packed), BF16),
            pltpu.VMEM(packed, F32),
            pltpu.VMEM(packed, BF16),
            pltpu.VMEM(packed, BF16),
            pltpu.VMEM(packed, BF16),
            pltpu.VMEM((regions + 2, *packed), BF16),
            dma((regions,)),
            dma((6,)),
            dma((4,)),
            dma((4,)),
            dma((2,)),
            dma((2,)),
            dma,
            dma,
            dma((9,)),
            dma((regions + 2,)),
        ],
        compiler_params=pltpu.CompilerParams(
            collective_id=0, has_side_effects=True, vmem_limit_bytes=67043328 - 7208960
        ),
        name="assimilate",
    )(obs_count, radius, obs, innovation, error_weight, obs_column, shaped)
    result = pl.pallas_call(
        finish,
        out_shape=jax.ShapeDtypeStruct(shaped.shape, BF16),
        in_specs=[vmem] * 4,
        out_specs=hbm,
        scratch_shapes=[
            pltpu.VMEM((lags, 2, shaped.shape[2] // 2, members), BF16),
            dma((lags, regions, 2)),
        ],
        compiler_params=pltpu.CompilerParams(vmem_limit_bytes=32 << 20),
        name="finish",
    )(*parts)
    return result.reshape(states.shape)


def solution(mesh):
    return jax.shard_map(
        functools.partial(shards, mesh.shape["tm"], mesh.shape["space"]),
        mesh=mesh,
        in_specs=(
            P("tm", "space", None, None),
            P("tm", "space", None),
            P("tm", "space", None),
            P("tm", "space", None),
            P("tm", "space"),
            P("space"),
            P("tm", "space", None, None),
        ),
        out_specs=P("tm", "space", None, None),
        check_vma=False,
    )
```
